16 devices in a mesh: tp: 4 (over z, y), cp: 4 (over x, core).
Axes of the slice: x: 2, y: 2, z: 2, core: 2. Of those that a mesh axis runs over, the one named last changes fastest.
Arguments:
- x_in: bfloat16 [12, 1536, 2304], P(None, 'cp')
- positions: int32 [1536], P('cp')
- rope_cos: float32 [1536, 256], P('cp')
- rope_sin: float32 [1536, 256], P('cp')
- norm_a: bfloat16 [2304], replicated
- wq_a: bfloat16 [2304, 2048], P(None, 'tp')
- wk_a: bfloat16 [2304, 1024], P(None, 'tp')
- wv_a: bfloat16 [2304, 1024], P(None, 'tp')
- wo_a: bfloat16 [2048, 2304], P('tp')
- norm_b: bfloat16 [2304], replicated
- wq_b: bfloat16 [2304, 2048], P(None, 'tp')
- wk_b: bfloat16 [2304, 1024], P(None, 'tp')
- wv_b: bfloat16 [2304, 1024], P(None, 'tp')
- wo_b: bfloat16 [2048, 2304], P('tp')
- grad_y: bfloat16 [12, 1536, 2304], P(None, 'cp')
Outputs:
- output 1: bfloat16 [12, 1536, 2304], P(None, 'cp')
- output 2: bfloat16 [12, 1536, 2304], P(None, 'cp')
- output 3: bfloat16 [2304], P('cp')
- output 4: bfloat16 [2304, 2048], P('cp', 'tp')
- output 5: bfloat16 [2304, 1024], P('cp', 'tp')
- output 6: bfloat16 [2304, 1024], P('cp', 'tp')
- output 7: bfloat16 [2048, 2304], P(('tp', 'cp'))
- output 8: bfloat16 [2304], P('cp')
- output 9: bfloat16 [2304, 2048], P('cp', 'tp')
- output 10: bfloat16 [2304, 1024], P('cp', 'tp')
- output 11: bfloat16 [2304, 1024], P('cp', 'tp')
- output 12: bfloat16 [2048, 2304], P(('tp', 'cp'))
All inputs are finite; a program needn't handle non-finite values.
Results may differ from the reference program's by a relative error of at most 0.02.
Values are sent between devices in bfloat16 or wider.
A program may use at most 1 GiB of HBM per device.

```python
import jax
import jax.numpy as jnp
from jax import lax

BATCH = 12
SEQ_LEN = 1536
D_MODEL = 2304
Q_HEADS = 8
KV_HEADS = 4
HEAD_DIM = 256
REF_ROWS = 128

CHUNK = 2 ** 13
ROPE_BASE = 500000.0
NORM_EPS = 1e-5
QK_EPS = 1e-6
TEMP_SCALE = 0.1
NEG_BIG = -1e30


def draw_positions(key):
    key_chunk, key_shift = jax.random.split(key)
    chunk_no = jax.random.randint(key_chunk, (), 2, 6)
    shift = jax.random.randint(key_shift, (), 1, min(SEQ_LEN, CHUNK))
    return (chunk_no * CHUNK - shift + jnp.arange(SEQ_LEN)).astype(jnp.int32)


def rope_tables(positions):
    half = HEAD_DIM // 2
    inv_freq = ROPE_BASE ** (-(jnp.arange(half).astype(jnp.float32) * 2.0 / HEAD_DIM))
    angles = positions.astype(jnp.float32)[:, None] * inv_freq[None, :]
    angles = jnp.concatenate([angles, angles], axis=1)
    return jnp.cos(angles), jnp.sin(angles)


def setup_inputs(seed: int = 0) -> dict:
    keys = jax.random.split(jax.random.key(seed), 16)
    positions = draw_positions(keys[0])
    rope_cos, rope_sin = rope_tables(positions)
    q_width = Q_HEADS * HEAD_DIM
    kv_width = KV_HEADS * HEAD_DIM
    act_shape = (BATCH, SEQ_LEN, D_MODEL)

    def weight(sub_key, rows, cols):
        return (jax.random.normal(sub_key, (rows, cols), jnp.float32) * rows ** -0.5).astype(jnp.bfloat16)

    def gain(sub_key):
        return jax.random.uniform(sub_key, (D_MODEL,), jnp.float32, 0.5, 1.5).astype(jnp.bfloat16)

    return {
        'x_in': jax.random.normal(keys[1], act_shape, jnp.float32).astype(jnp.bfloat16),
        'positions': positions,
        'rope_cos': rope_cos,
        'rope_sin': rope_sin,
        'norm_a': gain(keys[3]),
        'wq_a': weight(keys[4], D_MODEL, q_width),
        'wk_a': weight(keys[5], D_MODEL, kv_width),
        'wv_a': weight(keys[6], D_MODEL, kv_width),
        'wo_a': weight(keys[7], q_width, D_MODEL),
        'norm_b': gain(keys[8]),
        'wq_b': weight(keys[9], D_MODEL, q_width),
        'wk_b': weight(keys[10], D_MODEL, kv_width),
        'wv_b': weight(keys[11], D_MODEL, kv_width),
        'wo_b': weight(keys[12], q_width, D_MODEL),
        'grad_y': jax.random.normal(keys[2], act_shape, jnp.float32).astype(jnp.bfloat16),
    }


def rms_norm(act, gamma):
    act_wide = act.astype(jnp.float32)
    inv_rms = lax.rsqrt(jnp.mean(act_wide * act_wide, axis=-1, keepdims=True) + NORM_EPS)
    return (act_wide * inv_rms * gamma.astype(jnp.float32)).astype(jnp.bfloat16)


def project(act, weight):
    rows = act.shape[0] * act.shape[1]
    flat = jnp.dot(act.reshape(rows, act.shape[2]), weight, preferred_element_type=jnp.float32)
    return flat.reshape(act.shape[0], act.shape[1], weight.shape[1]).astype(jnp.bfloat16)


def rotate(wide, cos_tab, sin_tab):
    half = HEAD_DIM // 2
    turned = jnp.concatenate([-wide[..., half:], wide[..., :half]], axis=-1)
    return wide * cos_tab[None, :, None, :] + turned * sin_tab[None, :, None, :]


def qk_prep(raw_val, cos_tab, sin_tab):
    wide = rotate(raw_val.astype(jnp.float32), cos_tab, sin_tab)
    return (wide * lax.rsqrt(jnp.mean(wide * wide, axis=-1, keepdims=True) + QK_EPS)).astype(jnp.bfloat16)


def temperature(positions):
    return jnp.log(((positions + 1) // CHUNK).astype(jnp.float32) + 1.0) * TEMP_SCALE + 1.0


def attention(queries, keys, values, positions, local):
    scale = HEAD_DIM ** -0.5
    groups = Q_HEADS // KV_HEADS
    n_blocks = SEQ_LEN // REF_ROWS

    def block_attend(q_rows, q_pos, keys_wide, vals_wide, key_pos):
        scores = jnp.einsum('bqkgd,bskd->bkgqs', q_rows.astype(jnp.float32), keys_wide) * scale
        allowed = key_pos[None, :] <= q_pos[:, None]
        if local:
            allowed = jnp.logical_and(allowed, (key_pos // CHUNK)[None, :] == (q_pos // CHUNK)[:, None])
        attn_prob = jax.nn.softmax(jnp.where(allowed, scores, NEG_BIG), axis=-1).astype(jnp.bfloat16)
        attn_out = jnp.einsum('bkgqs,bskd->bqkgd', attn_prob.astype(jnp.float32), vals_wide)
        return attn_out.astype(jnp.bfloat16)

    keys_wide = keys.astype(jnp.float32)
    vals_wide = values.astype(jnp.float32)
    attend = jax.checkpoint(block_attend)

    def one_block(block_in):
        return attend(block_in[0], block_in[1], keys_wide, vals_wide, positions)

    q_blocks = jnp.moveaxis(queries.reshape(BATCH, n_blocks, REF_ROWS, KV_HEADS, groups, HEAD_DIM), 1, 0)
    block_outs = lax.map(one_block, (q_blocks, positions.reshape(n_blocks, REF_ROWS)))
    return jnp.moveaxis(block_outs, 0, 1).reshape(BATCH, SEQ_LEN, Q_HEADS * HEAD_DIM)


def forward(x_in, positions, rope_cos, rope_sin, norm_a, wq_a, wk_a, wv_a, wo_a, norm_b, wq_b, wk_b, wv_b, wo_b):
    q_shape = (BATCH, SEQ_LEN, KV_HEADS, Q_HEADS // KV_HEADS, HEAD_DIM)
    kv_shape = (BATCH, SEQ_LEN, KV_HEADS, HEAD_DIM)
    xn_a = rms_norm(x_in, norm_a)
    query_a = qk_prep(project(xn_a, wq_a).reshape(BATCH, SEQ_LEN, Q_HEADS, HEAD_DIM), rope_cos, rope_sin).reshape(q_shape)
    key_a = qk_prep(project(xn_a, wk_a).reshape(kv_shape), rope_cos, rope_sin)
    value_a = project(xn_a, wv_a).reshape(kv_shape)
    out_a = attention(query_a, key_a, value_a, positions, True)
    h_mid = (x_in.astype(jnp.float32) + project(out_a, wo_a).astype(jnp.float32)).astype(jnp.bfloat16)
    xn_b = rms_norm(h_mid, norm_b)
    q_temp = temperature(positions)[None, :, None]
    query_b = (project(xn_b, wq_b).astype(jnp.float32) * q_temp).astype(jnp.bfloat16).reshape(q_shape)
    key_b = project(xn_b, wk_b).reshape(kv_shape)
    value_b = project(xn_b, wv_b).reshape(kv_shape)
    out_b = attention(query_b, key_b, value_b, positions, False)
    return (h_mid.astype(jnp.float32) + project(out_b, wo_b).astype(jnp.float32)).astype(jnp.bfloat16)


def reference(x_in, positions, rope_cos, rope_sin, norm_a, wq_a, wk_a, wv_a, wo_a, norm_b, wq_b, wk_b, wv_b, wo_b, grad_y):
    def layers(x_arg, gain_a, w_qa, w_ka, w_va, w_oa, gain_b, w_qb, w_kb, w_vb, w_ob):
        return forward(x_arg, positions, rope_cos, rope_sin, gain_a, w_qa, w_ka, w_va, w_oa, gain_b, w_qb, w_kb, w_vb, w_ob)

    out_y, pullback = jax.vjp(layers, x_in, norm_a, wq_a, wk_a, wv_a, wo_a, norm_b, wq_b, wk_b, wv_b, wo_b)
    grads = pullback(grad_y)
    return (out_y, grads[0], grads[1], grads[2], grads[3], grads[4], grads[5], grads[6], grads[7], grads[8], grads[9], grads[10])
```

```python
import functools

import jax
import jax.numpy as jnp
from jax import lax
from jax.experimental import pallas as pl
from jax.experimental.pallas import tpu as pltpu
from jax.sharding import PartitionSpec as P

CHUNK = 8192
NORM_EPS = 1e-5
QK_EPS = 1e-6
TEMP_SCALE = 0.1
NEG_BIG = -1e30
BLK = 384
HEAD = 256
HALF = 128
SCALE = 0.0625
F32 = jnp.float32
BF16 = jnp.bfloat16


COORDS = [(z, y, x, c) for z in range(2) for y in range(2) for x in range(2) for c in range(2)]


def dev(z, y, x, c):
    return (2 * z + y) * 4 + 2 * x + c


def pairs(target, only=lambda z, y, x, c: True):
    return [(dev(*co), dev(*target(*co))) for co in COORDS if only(*co)]


CORE_SWAP = pairs(lambda z, y, x, c: (z, y, x, 1 - c))
X_SWAP = pairs(lambda z, y, x, c: (z, y, 1 - x, c))
XC_SWAP = pairs(lambda z, y, x, c: (z, y, 1 - x, 1 - c))
Y_SWAP = pairs(lambda z, y, x, c: (z, 1 - y, x, c))
X_SWAP0 = pairs(lambda z, y, x, c: (z, y, 1 - x, c), lambda z, y, x, c: c == 0)
Y_SWAP0 = pairs(lambda z, y, x, c: (z, 1 - y, x, c), lambda z, y, x, c: c == 0)
KV_FORWARD = pairs(lambda z, y, x, c: (z, y, 1, c), lambda z, y, x, c: x == 0)
KV_BACK = pairs(lambda z, y, x, c: (z, y, 0, c), lambda z, y, x, c: x == 1)
W_FIRST = pairs(lambda z, y, x, c: (z, 1 - y, x, 0) if c == 0 else (1 - z, y, x, 1))
W_VIA_Z = pairs(lambda z, y, x, c: (1 - z, y, x, 1), lambda z, y, x, c: c == 0)
W_VIA_Y = pairs(lambda z, y, x, c: (z, 1 - y, x, 1), lambda z, y, x, c: c == 1)
Z_HOME = pairs(lambda z, y, x, c: (1 - z, y, x, 0), lambda z, y, x, c: c == 1)
CORE_SPREAD = pairs(lambda z, y, x, c: (z, y, x, 1), lambda z, y, x, c: c == 0)
AXES = ('tp', 'cp')


def permute(val, perm):
    return lax.ppermute(val, AXES, perm)


NT = (((1,), (1,)), ((), ()))
NN = (((1,), (0,)), ((), ()))


def dot32(lhs, rhs, dims):
    return lax.dot_general(lhs, rhs, dims, preferred_element_type=F32)


def turn(raw, tab):
    wide = raw.astype(F32)
    lo, hi = wide[:, :HALF], wide[:, HALF:]
    cos_t, sin_t = tab[:, :HALF], tab[:, HALF:]
    t_lo = lo * cos_t - hi * sin_t
    t_hi = hi * cos_t + lo * sin_t
    mean_sq = jnp.sum(t_lo * t_lo + t_hi * t_hi, axis=-1, keepdims=True) * (1.0 / HEAD)
    return t_lo, t_hi, lax.rsqrt(mean_sq + QK_EPS)


def prep(raw, tab):
    t_lo, t_hi, inv = turn(raw, tab)
    return jnp.concatenate([(t_lo * inv).astype(BF16), (t_hi * inv).astype(BF16)], axis=1)


def prep_back(raw, tab, grad):
    t_lo, t_hi, inv = turn(raw, tab)
    g_wide = grad.astype(BF16).astype(F32)
    g_lo, g_hi = g_wide[:, :HALF], g_wide[:, HALF:]
    n_lo, n_hi = t_lo * inv, t_hi * inv
    mean_g = jnp.sum(g_lo * n_lo + g_hi * n_hi, axis=-1, keepdims=True) * (1.0 / HEAD)
    d_lo = inv * (g_lo - n_lo * mean_g)
    d_hi = inv * (g_hi - n_hi * mean_g)
    cos_t, sin_t = tab[:, :HALF], tab[:, HALF:]
    return jnp.concatenate([(d_lo * cos_t + d_hi * sin_t).astype(BF16),
                            (d_hi * cos_t - d_lo * sin_t).astype(BF16)], axis=1)


def seq_block(split, step, x_idx, c_idx):
    if split:
        return 2 * x_idx + (c_idx + step) % 2
    return 2 * ((x_idx + step % 2) % 2) + (c_idx + step // 2) % 2


def tab_row(split, step):
    return 2 * step if split else step


def query_rows(local, q_ref, tab_ref, row):
    halves = []
    tab = tab_ref[pl.ds(row * BLK, BLK), :]
    for head in range(2):
        raw = q_ref[:, head * HEAD:(head + 1) * HEAD]
        if local:
            ready = prep(raw, tab)
        else:
            wide = raw.astype(F32)
            ready = jnp.concatenate([(wide[:, :HALF] * tab).astype(BF16),
                                     (wide[:, HALF:] * tab).astype(BF16)], axis=1)
        halves.append(ready)
    return jnp.concatenate(halves, axis=0) * jnp.asarray(SCALE, BF16)


def load_keys(local, split, n_blocks, x_idx, c_idx, k_ref, v_ref, kx_ref, vx_ref, tab_ref, put):
    def one(src_k, src_v, row, block, tab_block):
        raw = src_k[row * BLK:(row + 1) * BLK, :]
        if local:
            raw = prep(raw, tab_ref[tab_block * BLK:(tab_block + 1) * BLK, :])
        put(block, raw, src_v[row * BLK:(row + 1) * BLK, :])

    for step in range(n_blocks):
        one(k_ref, v_ref, step, seq_block(split, step, x_idx, c_idx), tab_row(split, step))
    if split:
        @pl.when(x_idx == 1)
        def _():
            for step in range(2):
                one(kx_ref, vx_ref, step, (c_idx + step) % 2, 1 + 2 * step)


def mask_of(block, n_block, first):
    key_pos = block * BLK + lax.broadcasted_iota(jnp.int32, (BLK, 2 * BLK), 0)
    lane = lax.broadcasted_iota(jnp.int32, (1, 2 * BLK), 1)
    q_pos = n_block * BLK + jnp.where(lane >= BLK, lane - BLK, lane)
    low = jnp.where(q_pos >= first, first, 0)
    return (key_pos >= low) & (key_pos <= q_pos)


def fwd_kernel(local, split, n_blocks, info, *refs):
    if split:
        q_ref, k_ref, v_ref, kx_ref, vx_ref, tab_ref, o_ref, lse_ref, kp, vt, sc, acc = refs
    else:
        q_ref, k_ref, v_ref, tab_ref, o_ref, lse_ref, kp, vt, sc, acc = refs
        kx_ref = vx_ref = None
    x_idx, c_idx, first = info[0], info[1], info[2]
    step = pl.program_id(1)
    n_block = seq_block(split, step, x_idx, c_idx)

    @pl.when(step == 0)
    def _():
        def put(block, keys, vals):
            kp[block] = keys
            vt[block] = vals.T
        load_keys(local, split, n_blocks, x_idx, c_idx, k_ref, v_ref, kx_ref, vx_ref, tab_ref, put)

    query = query_rows(local, q_ref, tab_ref, tab_row(split, step))
    start = jnp.where(n_block * BLK >= first, first // BLK, 0)

    def scores(block, row_max):
        val = dot32(kp[block], query, NT)
        sc[block] = val

        @pl.when((block == n_block) | ((block * BLK < first) & ((n_block + 1) * BLK > first)))
        def _():
            sc[block] = jnp.where(mask_of(block, n_block, first), sc[block], NEG_BIG)
        return jnp.maximum(row_max, jnp.max(sc[block], axis=0, keepdims=True))

    row_max = lax.fori_loop(start, n_block + 1, scores, jnp.full((1, 2 * BLK), NEG_BIG, F32))

    def total(block, row_sum):
        return row_sum + jnp.sum(jnp.exp(sc[block] - row_max), axis=0, keepdims=True)

    row_sum = lax.fori_loop(start, n_block + 1, total, jnp.zeros((1, 2 * BLK), F32))
    lse = row_max + jnp.log(row_sum)
    acc[...] = jnp.zeros_like(acc)

    def gather(block, carry):
        prob = jnp.exp(sc[block] - lse).astype(BF16)
        acc[...] += dot32(vt[block], prob, NN)
        return carry

    lax.fori_loop(start, n_block + 1, gather, 0)
    out = acc[...].T.astype(BF16)
    o_ref[...] = jnp.concatenate([out[:BLK], out[BLK:]], axis=1)
    lse_ref[...] = jnp.broadcast_to(lse, (8, 2 * BLK)).reshape(1, 1, 8, 2 * BLK)


def bwd_kernel(local, split, n_blocks, info, *refs):
    if split:
        (q_ref, k_ref, v_ref, kx_ref, vx_ref, tab_ref, o_ref, do_ref, lse_ref,
         dq_ref, dkv_ref, dkvx_ref, kp, kt, vp, dk, dv, dqt) = refs
    else:
        (q_ref, k_ref, v_ref, tab_ref, o_ref, do_ref, lse_ref,
         dq_ref, dkv_ref, kp, kt, vp, dk, dv, dqt) = refs
        kx_ref = vx_ref = None
    x_idx, c_idx, first = info[0], info[1], info[2]
    step = pl.program_id(1)
    n_block = seq_block(split, step, x_idx, c_idx)

    @pl.when(step == 0)
    def _():
        def put(block, keys, vals):
            kp[block] = keys
            kt[block] = keys.T
            vp[block] = vals
        load_keys(local, split, n_blocks, x_idx, c_idx, k_ref, v_ref, kx_ref, vx_ref, tab_ref, put)
        dk[...] = jnp.zeros_like(dk)
        dv[...] = jnp.zeros_like(dv)

    query = query_rows(local, q_ref, tab_ref, tab_row(split, step))
    d_out = jnp.concatenate([do_ref[:, :HEAD], do_ref[:, HEAD:]], axis=0)
    out = jnp.concatenate([o_ref[:, :HEAD], o_ref[:, HEAD:]], axis=0)
    prod = d_out.astype(F32) * out.astype(F32)
    delta = jnp.sum((prod[:, :HALF] + prod[:, HALF:]).T, axis=0, keepdims=True)
    lse = lse_ref[0, 0, 0:1, :]
    start = jnp.where(n_block * BLK >= first, first // BLK, 0)
    dqt[...] = jnp.zeros_like(dqt)

    def one(block, masked):
        prob = jnp.exp(dot32(kp[block], query, NT) - lse)
        if masked:
            prob = jnp.where(mask_of(block, n_block, first), prob, 0.0)
        d_prob = dot32(vp[block], d_out, NT)
        d_score = (prob * (d_prob - delta)).astype(BF16)
        dv[block] += dot32(prob.astype(BF16), d_out, NN)
        dk[block] += dot32(d_score, query, NN)
        dqt[...] += dot32(kt[block], d_score, NN)

    def loop(block, carry):
        edge = (block == n_block) | ((block * BLK < first) & ((n_block + 1) * BLK > first))
        pl.when(edge)(lambda: one(block, True))
        pl.when(jnp.logical_not(edge))(lambda: one(block, False))
        return carry

    lax.fori_loop(start, n_block + 1, loop, 0)
    d_query = dqt[...].T * SCALE
    row = tab_row(split, step)
    tab = tab_ref[pl.ds(row * BLK, BLK), :]
    for head in range(2):
        grad = d_query[head * BLK:(head + 1) * BLK]
        cols = slice(head * HEAD, (head + 1) * HEAD)
        if local:
            dq_ref[:, cols] = prep_back(q_ref[:, cols], tab, grad)
        else:
            dq_ref[:, cols] = jnp.concatenate([(grad[:, :HALF] * tab).astype(BF16),
                                               (grad[:, HALF:] * tab).astype(BF16)], axis=1)

    @pl.when(step == n_blocks - 1)
    def _():
        def emit(dst, src_k, at, block, tab_block):
            rows = slice(at * BLK, (at + 1) * BLK)
            grad = dk[block]
            if local:
                grad = prep_back(src_k[rows, :], tab_ref[tab_block * BLK:(tab_block + 1) * BLK, :], grad)
            dst[rows, :HEAD] = grad.astype(BF16)
            dst[rows, HEAD:] = dv[block].astype(BF16)

        for at in range(n_blocks):
            emit(dkv_ref, k_ref, at, seq_block(split, at, x_idx, c_idx), tab_row(split, at))
        if split:
            @pl.when(x_idx == 1)
            def _():
                for at in range(2):
                    emit(dkvx_ref, kx_ref, at, (c_idx + at) % 2, 1 + 2 * at)

            @pl.when(x_idx == 0)
            def _():
                dkvx_ref[...] = jnp.zeros_like(dkvx_ref)


def attn_specs(local, split, n_blocks):
    rows = n_blocks * BLK
    specs = [pl.BlockSpec((BLK, 2 * HEAD), lambda s, i, info: (i, s)),
             pl.BlockSpec((rows, HEAD), lambda s, i, info: (0, 4 + 2 * s)),
             pl.BlockSpec((rows, HEAD), lambda s, i, info: (0, 5 + 2 * s))]
    if split:
        specs += [pl.BlockSpec((rows, HEAD), lambda s, i, info: (0, 2 * s)),
                  pl.BlockSpec((rows, HEAD), lambda s, i, info: (0, 2 * s + 1))]
    specs.append(pl.BlockSpec((4 * BLK, HEAD if local else HALF), lambda s, i, info: (0, 0)))
    return specs


def attn_cost(split, matmuls):
    pairs_done = (7 if split else 10) * 4
    return pl.CostEstimate(flops=pairs_done * matmuls * 2 * BLK * BLK * HEAD,
                           bytes_accessed=16 << 20, transcendentals=pairs_done * 2 * BLK * BLK)


def attn_forward(local, split, info, qkv, kvx, table):
    n_blocks = 2 if split else 4
    rows = n_blocks * BLK
    operands = [qkv, qkv, qkv] + ([kvx, kvx] if split else []) + [table]
    return pl.pallas_call(
        functools.partial(fwd_kernel, local, split, n_blocks),
        grid_spec=pltpu.PrefetchScalarGridSpec(
            num_scalar_prefetch=1, grid=(2, n_blocks),
            in_specs=attn_specs(local, split, n_blocks),
            out_specs=[pl.BlockSpec((BLK, 2 * HEAD), lambda s, i, info: (i, s)),
                       pl.BlockSpec((1, 1, 8, 2 * BLK), lambda s, i, info: (s, i, 0, 0))],
            scratch_shapes=[pltpu.VMEM((4, BLK, HEAD), BF16), pltpu.VMEM((4, HEAD, BLK), BF16),
                            pltpu.VMEM((4, BLK, 2 * BLK), F32), pltpu.VMEM((HEAD, 2 * BLK), F32)]),
        out_shape=[jax.ShapeDtypeStruct((rows, 4 * HEAD), BF16),
                   jax.ShapeDtypeStruct((2, n_blocks, 8, 2 * BLK), F32)],
        cost_estimate=attn_cost(split, 2),
        name=('local' if local else 'global') + ('_split' if split else '_whole') + '_fwd',
    )(info, *operands)


def attn_backward(local, split, info, qkv, kvx, table, out, d_out, lse):
    n_blocks = 2 if split else 4
    rows = n_blocks * BLK
    operands = [qkv, qkv, qkv] + ([kvx, kvx] if split else []) + [table, out, d_out, lse]
    out_specs = [pl.BlockSpec((BLK, 2 * HEAD), lambda s, i, info: (i, s)),
                 pl.BlockSpec((rows, 2 * HEAD), lambda s, i, info: (0, s))]
    out_shape = [jax.ShapeDtypeStruct((rows, 4 * HEAD), BF16)] * 2
    if split:
        out_specs.append(out_specs[1])
        out_shape.append(out_shape[1])
    return pl.pallas_call(
        functools.partial(bwd_kernel, local, split, n_blocks),
        grid_spec=pltpu.PrefetchScalarGridSpec(
            num_scalar_prefetch=1, grid=(2, n_blocks),
            in_specs=attn_specs(local, split, n_blocks) + [
                pl.BlockSpec((BLK, 2 * HEAD), lambda s, i, info: (i, s)),
                pl.BlockSpec((BLK, 2 * HEAD), lambda s, i, info: (i, s)),
                pl.BlockSpec((1, 1, 8, 2 * BLK), lambda s, i, info: (s, i, 0, 0))],
            out_specs=out_specs,
            scratch_shapes=[pltpu.VMEM((4, BLK, HEAD), BF16), pltpu.VMEM((4, HEAD, BLK), BF16),
                            pltpu.VMEM((4, BLK, HEAD), BF16), pltpu.VMEM((4, BLK, HEAD), F32),
                            pltpu.VMEM((4, BLK, HEAD), F32), pltpu.VMEM((HEAD, 2 * BLK), F32)]),
        out_shape=out_shape,
        cost_estimate=attn_cost(split, 5),
        name=('local' if local else 'global') + ('_split' if split else '_whole') + '_bwd',
    )(info, *operands)


def rms_norm(act, gamma):
    act_wide = act.astype(F32)
    inv_rms = lax.rsqrt(jnp.mean(act_wide * act_wide, axis=-1, keepdims=True) + NORM_EPS)
    return (act_wide * inv_rms * gamma.astype(F32)).astype(BF16)


def norm_backward(act, gamma, grad_out):
    act_wide = act.astype(F32)
    inv_rms = lax.rsqrt(jnp.mean(act_wide * act_wide, axis=-1, keepdims=True) + NORM_EPS)
    x_hat = act_wide * inv_rms
    grad_gain = jnp.sum(grad_out * x_hat, axis=0)
    grad_hat = grad_out * gamma.astype(F32)
    grad_act = inv_rms * (grad_hat - x_hat * jnp.mean(grad_hat * x_hat, axis=-1, keepdims=True))
    return grad_act, grad_gain


def mm(lhs, rhs):
    return dot32(lhs, rhs, NN)


def mm_t(lhs, rhs):
    return dot32(lhs, rhs, NT)


def mm_tn(lhs, rhs):
    return dot32(lhs, rhs, (((0,), (0,)), ((), ())))


def after(val, *done):
    return lax.optimization_barrier((val,) + done)[0]


def solution(mesh):
    row_spec = P(None, 'cp', None)
    col_spec = P(None, 'tp')
    grid_spec = P('cp', 'tp')
    out_rows = P(('tp', 'cp'), None)
    in_specs = (row_spec, P('cp'), P('cp', None), P('cp', None),
                P(None), col_spec, col_spec, col_spec, P('tp', None),
                P(None), col_spec, col_spec, col_spec, P('tp', None), row_spec)
    out_specs = (row_spec, row_spec,
                 P('cp'), grid_spec, grid_spec, grid_spec, out_rows,
                 P('cp'), grid_spec, grid_spec, grid_spec, out_rows)

    def body(x_in, positions, rope_cos, rope_sin, norm_a, wq_a, wk_a, wv_a, wo_a,
             norm_b, wq_b, wk_b, wv_b, wo_b, grad_y):
        width = x_in.shape[2]
        half_w = width // 2
        t_idx = lax.axis_index('tp')
        r_idx = lax.axis_index('cp')
        x_idx, c_idx = r_idx // 2, r_idx % 2
        is_c0 = c_idx == 0
        pos_0 = positions[0] - r_idx * BLK
        info_a = jnp.stack([x_idx, c_idx, CHUNK - pos_0 % CHUNK]).astype(jnp.int32)
        info_b = jnp.stack([x_idx, c_idx, jnp.int32(1 << 24)]).astype(jnp.int32)

        table = jnp.concatenate([rope_cos[:, :HALF], rope_sin[:, :HALF]], axis=1)
        table = jnp.concatenate([table, permute(table, X_SWAP), permute(table, CORE_SWAP),
                                 permute(table, XC_SWAP)], axis=0)
        blocks = jnp.stack([seq_block(False, i, x_idx, c_idx) for i in range(4)])
        seq_pos = pos_0 + (blocks[:, None] * BLK + jnp.arange(BLK)[None, :]).reshape(-1)
        tau = jnp.log(((seq_pos + 1) // CHUNK).astype(F32) + 1.0) * TEMP_SCALE + 1.0
        tau = jnp.broadcast_to(tau[:, None], (4 * BLK, HALF))

        def take(arr, batch):
            return lax.dynamic_index_in_dim(arr, batch, 0, keepdims=False)

        def pick(arr):
            away = permute(take(arr, 3 * t_idx + 1 - x_idx), X_SWAP)
            whole = jnp.concatenate([take(arr, 3 * t_idx + x_idx), away], axis=0)
            return whole, take(arr, 3 * t_idx + 2)

        def both_cores(whole, shared):
            return jnp.concatenate([whole, permute(whole, CORE_SWAP), shared, permute(shared, CORE_SWAP)], axis=0)

        n_whole = 4 * BLK

        def gather_shard(shard):
            first = permute(shard, W_FIRST)
            mid = shard.shape[0] // 2
            last = jnp.concatenate([permute(first[:mid], W_VIA_Z), permute(first[mid:], W_VIA_Y)], axis=0)
            own = jnp.where(is_c0, shard, first)
            oth = jnp.where(is_c0, first, last)
            return own, oth

        def gather_qkv(wq, wk, wv):
            own, oth = gather_shard(jnp.concatenate([wq, wk, wv], axis=1))
            split = wq.shape[1]
            return jnp.concatenate([own[:, :split], oth[:, :split], own[:, split:], oth[:, split:]], axis=1)

        def gather_o(wo):
            own, oth = gather_shard(wo)
            return jnp.concatenate([own, oth], axis=0)

        w_a = gather_qkv(wq_a, wk_a, wv_a)
        o_a = gather_o(after(wo_a, w_a))
        w_b = gather_qkv(*lax.optimization_barrier((wq_b, wk_b, wv_b, o_a))[:3])
        o_b = gather_o(after(wo_b, w_b))

        def sublayer(local, act, gain, w_qkv, w_o, table_l, info):
            x_norm = both_cores(rms_norm(act[0], gain), rms_norm(act[1], gain))
            qkv_s = mm(x_norm[n_whole:], w_qkv).astype(BF16)
            kvx = permute(qkv_s[:, 4 * HEAD:], KV_FORWARD)
            qkv_w = mm(x_norm[:n_whole], w_qkv).astype(BF16)
            out_w, lse_w = attn_forward(local, False, info, qkv_w, None, table_l)
            out_s, lse_s = attn_forward(local, True, info, qkv_s, kvx, table_l)

            def project(out, rest):
                keep = out.shape[0] // 2
                part = permute(mm(out[keep:], w_o).astype(BF16), CORE_SWAP)
                attn = (mm(out[:keep], w_o) + part.astype(F32)).astype(BF16)
                return (rest.astype(F32) + attn.astype(F32)).astype(BF16)

            nxt = (project(out_w, act[0]), project(out_s, act[1]))
            return nxt, (x_norm, qkv_w, qkv_s, kvx, out_w, out_s, lse_w, lse_s)

        x_own = pick(x_in)
        h_own, saved_a = sublayer(True, x_own, norm_a, w_a, o_a, table, info_a)
        y_own, saved_b = sublayer(False, h_own, norm_b, w_b, o_b, tau, info_b)

        def spread(whole, shared):
            mine, away = whole[:BLK], permute(whole[BLK:], X_SWAP)
            stack = jnp.stack([jnp.where(x_idx == 0, mine, away), jnp.where(x_idx == 0, away, mine), shared])
            return lax.all_gather(stack, 'tp', axis=0, tiled=True)

        out_y = spread(*y_own)

        def finish(total):
            rows = total.shape[0] // 2
            total = total.astype(BF16)
            return jnp.where(is_c0, total[:rows], permute(total[rows:], CORE_SPREAD))

        def rows_of(val, at, size):
            return lax.dynamic_slice_in_dim(val, at, size, 0)

        def cols_of(val, at, size):
            return lax.dynamic_slice_in_dim(val, at, size, 1)

        def reduce_o(out, grad):
            hw = HEAD

            def half(which):
                return mm_tn(jnp.concatenate([cols_of(out, which * hw, hw), cols_of(out, 2 * hw + which * hw, hw)], axis=1), grad)

            away = permute(half(1 - x_idx), X_SWAP)
            part = half(x_idx) + away
            part = part[:hw] + permute(part[hw:], Y_SWAP)
            return finish(part + permute(part, Z_HOME))

        def reduce_q(x_norm, grad):
            hw = 2 * HEAD
            away = permute(mm_tn(cols_of(x_norm, (1 - x_idx) * half_w, half_w), grad), X_SWAP)
            part = mm_tn(cols_of(x_norm, x_idx * half_w, half_w), grad) + away
            part = part[:, :hw] + permute(part[:, hw:], Y_SWAP)
            return finish(part + permute(part, Z_HOME))

        def reduce_kv(x_norm, grad):
            hw = 2 * HEAD
            part = mm_tn(x_norm, grad)
            part = part + permute(part, Z_HOME)
            away = permute(rows_of(part, (1 - x_idx) * half_w, half_w), X_SWAP0)
            part = rows_of(part, x_idx * half_w, half_w) + away
            part = finish(part[:, :hw] + permute(part[:, hw:], Y_SWAP0))
            return part[:, :HEAD], part[:, HEAD:]

        def sublayer_back(local, act, gain, w_qkv, w_o, table_l, info, saved, grad_own, grad_all):
            x_norm, qkv_w, qkv_s, kvx, out_w, out_s, lse_w, lse_s = saved
            d_out_s = mm_t(grad_all[n_whole:], w_o).astype(BF16)
            dq_s, dkv_s, dkvx = attn_backward(local, True, info, qkv_s, kvx, table_l, out_s, d_out_s, lse_s)
            back = permute(dkvx, KV_BACK)
            d_out_w = mm_t(grad_all[:n_whole], w_o).astype(BF16)
            dq_w, dkv_w = attn_backward(local, False, info, qkv_w, None, table_l, out_w, d_out_w, lse_w)
            dkv_s = (dkv_s.astype(F32) + back.astype(F32)).astype(BF16)
            d_w = jnp.concatenate([dq_w, dkv_w], axis=1)
            d_s = jnp.concatenate([dq_s, dkv_s], axis=1)

            def input_grad(d_qkv, act_own, grad_rows):
                keep = d_qkv.shape[0] // 2
                part = permute(mm_t(d_qkv[keep:], w_qkv).astype(BF16), CORE_SWAP)
                grad_norm = (mm_t(d_qkv[:keep], w_qkv) + part.astype(F32)).astype(BF16)
                grad_act, grad_gain = norm_backward(act_own, gain, grad_norm.astype(F32))
                return (grad_rows.astype(F32) + grad_act).astype(BF16), grad_gain

            new_w, gain_w = input_grad(d_w, act[0], grad_own[0])
            new_s, gain_s = input_grad(d_s, act[1], grad_own[1])
            grad_o = reduce_o(jnp.concatenate([out_w, out_s], axis=0), grad_all)
            grad_q = reduce_q(x_norm, jnp.concatenate([dq_w, dq_s], axis=0))
            grad_k, grad_v = reduce_kv(x_norm, jnp.concatenate([dkv_w, dkv_s], axis=0))
            return (new_w, new_s), gain_w + gain_s, (grad_q, grad_k, grad_v, grad_o)

        gy_own = pick(grad_y)
        gy_all = both_cores(*gy_own)
        gh_own, gain_b, grads_b = sublayer_back(False, h_own, norm_b, w_b, o_b, tau, info_b, saved_b, gy_own, gy_all)
        gx_own, gain_a, grads_a = sublayer_back(True, x_own, norm_a, w_a, o_a, table, info_a, saved_a,
                                                gh_own, both_cores(*gh_own))
        grad_x = spread(*gx_own)
        gains = lax.psum(jnp.stack([gain_a, gain_b]), AXES)
        gains = lax.dynamic_slice_in_dim(gains, r_idx * (width // 4), width // 4, 1).astype(BF16)
        return (out_y, grad_x, gains[0], *grads_a, gains[1], *grads_b)

    return jax.shard_map(body, mesh=mesh, in_specs=in_specs, out_specs=out_specs, check_vma=False)
```
